32 devices in a mesh: pipe: 4 (over y, x), dp: 8 (over z, core).
Axes of the slice: x: 2, y: 2, z: 4, core: 2. Of those that a mesh axis runs over, the one named last changes fastest.
Arguments:
- acts: bfloat16 [4, 2048, 3072], P('pipe', 'dp'), may hold values from -24 to 24, as said below
- grad: float32 [12288, 4096], P('pipe', 'dp'), may hold values from -6 to 6
- owner_of: int32 [4, 12], replicated, may hold values from 0 to 3, as said below
Outputs:
- precond: float32 [12288, 4096], P('pipe', 'dp')
- held_inverse: float32 [4, 24, 256, 256], P('pipe', None, 'dp')
The draws below stay inside these ranges and needn't reach their ends.
Inputs may be any that keep to these rules, and one draw needn't show every extreme that they name: `acts`: column and token scales of the activations vary; entries lie within the range. `owner_of`: no section index owns more than 24 blocks in all, and some section index owns exactly 24.
All inputs are finite; a program needn't handle non-finite values.
Results may differ from the reference program's by a relative error of at most 0.0003.
Values sent between devices are 32-bit elements; how exact they have to be, the bound alone decides.
A program may use at most 128 MiB of HBM per device.

```python
import math
import jax
import jax.numpy as jnp
from jax import lax

W = 3072
GO = 4096
BLK = 256
NB = 12
HOST = 24
TOKENS = 2048
N_PIPE = 4


def draw_acts(key, part):
    keys = jax.random.split(key, 3)
    shape = (N_PIPE, TOKENS, W)
    col_scale = jnp.exp(jax.random.uniform(keys[1], (N_PIPE, 1, W), jnp.float32, math.log(0.3), math.log(3.0)))
    row_scale = jnp.exp(jax.random.uniform(keys[2], (N_PIPE, TOKENS, 1), jnp.float32, math.log(0.5), math.log(2.0)))
    base = jax.random.normal(keys[0], shape, jnp.float32)
    base = jnp.clip(base, -4.0, 4.0)
    return (base * col_scale * row_scale).astype(jnp.bfloat16)


def draw_owner_of(key, part):
    keys = jax.random.split(jax.random.fold_in(key, 17), 3)
    slot_total = N_PIPE * HOST
    busiest = jax.random.randint(keys[0], (), 0, N_PIPE)
    scores = jax.random.permutation(keys[1], slot_total).astype(jnp.int32)
    slot_ids = jnp.arange(slot_total, dtype=jnp.int32)
    scores = jnp.where(slot_ids // HOST == busiest, scores - slot_total, scores)
    ordered = jnp.argsort(scores, stable=True).astype(jnp.int32)
    chosen = ordered[:N_PIPE * NB] // HOST
    mixing = jax.random.permutation(keys[2], N_PIPE * NB)
    return chosen[mixing].reshape(N_PIPE, NB).astype(jnp.int32)


def block_scale(rng, extent, shards, least, high):
    def one(axis_at, blocks):
        draws = jax.random.uniform(jax.random.fold_in(jax.random.fold_in(rng, 6), axis_at), (blocks,), jnp.float32, least / len(shards), high / len(shards))
        return jnp.repeat(jnp.exp(draws), extent[axis_at] // blocks).reshape((-1,) + (1,) * (len(extent) - axis_at - 1))

    level = one(*shards[0])
    for cut in shards[1:]:
        level = level * one(*cut)
    return level


def noise(stream_key, dims, scale, limit, cuts=(), held_as=jnp.bfloat16):
    result = scale * jax.random.normal(stream_key, dims, jnp.float32)
    if cuts:
        result = result * block_scale(stream_key, dims, cuts, -0.22, 0.18)
    return jnp.clip(result, -limit, limit).astype(held_as)


def setup_inputs(seed: int = 0) -> dict:
    arg_keys = jax.random.split(jax.random.key(seed), 4)
    return {
        "acts": draw_acts(jax.random.fold_in(arg_keys[3], 71), 0),
        "grad": noise(arg_keys[1], (N_PIPE * W, GO), 1.0, 6.0, ((0, 4), (1, 8)), jnp.float32),
        "owner_of": draw_owner_of(jax.random.fold_in(arg_keys[3], 71), 0),
    }


damping_ratio = 0.1

def invert_blocks(factor, vacant):
    order_size = factor.shape[-1]
    diagonal_sum = jnp.sum(jnp.diagonal(factor, axis1=1, axis2=2), axis=1)
    damping = damping_ratio * diagonal_sum / order_size
    identity = jnp.eye(order_size, dtype=factor.dtype)
    shifted = factor + (damping + vacant)[:, None, None] * identity
    cholesky_lower = jnp.linalg.cholesky(shifted)
    identity_stack = jnp.broadcast_to(identity, factor.shape)
    inv_lower = lax.linalg.triangular_solve(cholesky_lower, identity_stack, left_side=True, lower=True)
    return jnp.einsum('mkr,mkc->mrc', inv_lower, inv_lower, precision=lax.Precision.HIGHEST)

def slot_tables(owner_of):
    owners_flat = owner_of.reshape(-1).astype(jnp.int32)
    positions = jnp.arange(owners_flat.shape[0], dtype=jnp.int32)
    matches = owners_flat[:, None] == owners_flat[None, :]
    before = positions[None, :] < positions[:, None]
    slot_rank = jnp.sum((matches & before).astype(jnp.int32), axis=1)
    return (owners_flat, slot_rank)

def reference(acts, grad, owner_of):

    def per_section(section_acts):
        blocks = []
        for block_id in range(NB):
            columns = section_acts[:, block_id * BLK:(block_id + 1) * BLK]
            blocks.append(jnp.dot(columns.T.astype(jnp.float32), columns.astype(jnp.float32), preferred_element_type=jnp.float32))
        factor = jnp.stack(blocks) / TOKENS
        return invert_blocks(factor, jnp.zeros((NB,), factor.dtype))
    inverse = lax.map(per_section, acts)
    precond = jnp.einsum('sbrk,sbkc->sbrc', inverse, grad.reshape(N_PIPE, NB, BLK, GO), precision=lax.Precision.HIGHEST)
    precond = precond.reshape(N_PIPE * W, GO)
    owners_flat, slot_rank = slot_tables(owner_of)
    pipe_ids = jnp.arange(N_PIPE, dtype=jnp.int32)
    slot_ids = jnp.arange(HOST, dtype=jnp.int32)
    selector = (owners_flat[None, None, :] == pipe_ids[:, None, None]) & (slot_rank[None, None, :] == slot_ids[None, :, None])
    selector = selector.astype(inverse.dtype)
    held_inverse = jnp.einsum('pjk,krc->pjrc', selector, inverse.reshape(N_PIPE * NB, BLK, BLK), precision=lax.Precision.HIGHEST)
    return (precond, held_inverse)
```

```python
import functools

import jax
import jax.numpy as jnp
from jax import lax
from jax.experimental import pallas as pl
from jax.experimental.pallas import tpu as pltpu
from jax.sharding import PartitionSpec as P

BLK = 256
HALF = BLK // 2
PACK = HALF + 8
HOST = 24
MESH = pl.DeviceIdType.MESH

damping_ratio = 0.1
F32 = jnp.float32
BF16 = jnp.bfloat16
HIGHEST = lax.Precision.HIGHEST


def square_iota():
    rows = lax.broadcasted_iota(jnp.int32, (HALF, HALF), 0)
    cols = lax.broadcasted_iota(jnp.int32, (HALF, HALF), 1)
    return rows, cols


def pack_into(ref, m11, m21, m22):
    rows, cols = square_iota()
    diag = jnp.sum(jnp.where(rows == cols, m22, 0.0), axis=0, keepdims=True)
    ref[0:HALF, 0:HALF] = m21
    ref[0:HALF, HALF:BLK] = jnp.where(rows >= cols, m11, m22)
    ref[HALF:PACK, 0:HALF] = jnp.broadcast_to(diag, (PACK - HALF, HALF))
    ref[HALF:PACK, HALF:BLK] = jnp.zeros((PACK - HALF, HALF), F32)


def unpack(value):
    rows, cols = square_iota()
    m21 = value[0:HALF, 0:HALF]
    mixed = value[0:HALF, HALF:BLK]
    diag = value[HALF : HALF + 1, 0:HALF]
    turned = mixed.T
    m11 = jnp.where(rows >= cols, mixed, turned)
    m22 = jnp.where(rows < cols, mixed, jnp.where(rows == cols, diag, turned))
    return m11, m21, m22


def reduce_kernel(n, nhalf, nown, acts, out, theirs, mine, from_pair, from_chip, pair_s, pair_r, chip_s, chip_r):
    chips = n // 2
    me = lax.axis_index("dp")
    core = lax.rem(me, 2)
    chip = me // 2
    pair = me + 1 - 2 * core

    barrier = pltpu.get_barrier_semaphore()
    pl.semaphore_signal(barrier, inc=1, device_id={"dp": pair}, device_id_type=MESH)
    for step in range(1, chips):
        other = lax.rem(chip + step, chips) * 2 + core
        pl.semaphore_signal(barrier, inc=1, device_id={"dp": other}, device_id_type=MESH)
    pl.semaphore_wait(barrier, chips)

    def partial(block, ref):
        start = pl.multiple_of(block * BLK, BLK)
        x = acts[:, pl.ds(start, BLK)]
        full = lax.dot_general(x, x, (((0,), (0,)), ((), ())), preferred_element_type=F32)
        pack_into(ref, full[0:HALF, 0:HALF], full[HALF:BLK, 0:HALF], full[HALF:BLK, HALF:BLK])

    def pair_copy(t):
        return pltpu.make_async_remote_copy(
            src_ref=theirs.at[t], dst_ref=from_pair.at[t], send_sem=pair_s.at[t], recv_sem=pair_r.at[t],
            device_id={"dp": pair}, device_id_type=MESH,
        )

    @pl.loop(0, nhalf)
    def _(t):
        partial(2 * t + 1 - core, theirs.at[t])
        pair_copy(t).start()

    @pl.loop(0, nhalf)
    def _(t):
        partial(2 * t + core, mine.at[t])

    def chip_copy(t, slot, owner):
        return pltpu.make_async_remote_copy(
            src_ref=mine.at[t], dst_ref=from_chip.at[slot, chip], send_sem=chip_s.at[t],
            recv_sem=chip_r.at[slot, chip], device_id={"dp": owner * 2 + core}, device_id_type=MESH,
        )

    for t in range(nhalf):
        owner = t % chips
        pair_copy(t).wait()
        mine[t] = mine[t] + from_pair[t]

        @pl.when(chip != owner)
        def _():
            chip_copy(t, t // chips, owner).start()

    for slot in range(nown):
        t = slot * chips + chip

        @pl.when(t < nhalf)
        def _():
            total = mine[t]
            for step in range(1, chips):
                source = lax.rem(chip + step, chips)
                pltpu.make_async_remote_copy(
                    src_ref=from_chip.at[slot, source], dst_ref=from_chip.at[slot, source],
                    send_sem=chip_s.at[0], recv_sem=chip_r.at[slot, source],
                    device_id={"dp": source * 2 + core}, device_id_type=MESH,
                ).wait_recv()
                total = total + from_chip[slot, source]
            out[slot] = total

        @pl.when(t >= nhalf)
        def _():
            rows, cols = square_iota()
            eye = jnp.where(rows == cols, 1.0, 0.0)
            pack_into(out.at[slot], eye, jnp.zeros((HALF, HALF), F32), eye)

    for t in range(nhalf):
        owner = t % chips

        @pl.when(chip != owner)
        def _():
            chip_copy(t, t // chips, owner).wait_send()


def dot3(a, b, contract):
    return jnp.stack([
        lax.dot_general(a[i], b[i], (contract, ((), ())), precision=HIGHEST, preferred_element_type=F32)
        for i in range(a.shape[0])
    ])


def sweep_inverse(a):
    count = a.shape[0]
    panel_shape = (count, 8, HALF)
    sub = lax.broadcasted_iota(jnp.int32, panel_shape, 1)
    lane = lax.broadcasted_iota(jnp.int32, panel_shape, 2)
    all_lanes = lax.broadcasted_iota(jnp.int32, (count, HALF, HALF), 2)

    def panel(_, a):
        top = a[:, 0:8, :]
        cols = [jnp.broadcast_to(top[:, :, k : k + 1], panel_shape) for k in range(8)]
        lead = [jnp.broadcast_to(a[:, :, k : k + 1], a.shape) for k in range(8)]
        for k in range(8):
            here = cols[k]
            inv = jnp.broadcast_to(1.0 / here[:, k : k + 1, :], panel_shape)
            row = jnp.broadcast_to(top[:, k : k + 1, :], panel_shape) * inv
            at_row = sub == k
            new = jnp.where(at_row, row, top - here * row)
            edge = jnp.where(at_row, inv, -here * inv)
            top = jnp.where(lane == k, edge, new)
            for j in range(k + 1, 8):
                across = jnp.broadcast_to(cols[j][:, k : k + 1, :], panel_shape) * inv
                cols[j] = jnp.where(at_row, across, cols[j] - here * across)
        top = jnp.where(lane < 8, -top, top)
        rest = a
        for k in range(8):
            rest = rest - lead[k] * top[:, k : k + 1, :]
        tall = jnp.concatenate([top, jnp.zeros((count, HALF - 8, HALF), F32)], axis=1)
        turned = jnp.stack([tall[i].T for i in range(count)])
        rest = jnp.where(all_lanes < 8, turned, rest)
        a = jnp.concatenate([rest[:, 8:, :], top], axis=1)
        return pltpu.roll(a, HALF - 8, 2)

    return -lax.fori_loop(0, HALF // 8, panel, a)


def invert_kernel(tokens, packed, out):
    count = packed.shape[0]
    rows, cols = square_iota()
    parts = [unpack(packed[i] / tokens) for i in range(count)]
    m11 = jnp.stack([p[0] for p in parts])
    m21 = jnp.stack([p[1] for p in parts])
    m22 = jnp.stack([p[2] for p in parts])
    eye = rows == cols
    trace = jnp.sum(jnp.where(eye, m11 + m22, 0.0), axis=(1, 2), keepdims=True)
    damping = jnp.where(eye, damping_ratio * trace / BLK, 0.0)
    x11 = sweep_inverse(m11 + damping)
    g = dot3(m21, x11, ((1,), (0,)))
    schur = m22 + damping - dot3(g, m21, ((1,), (1,)))
    y = sweep_inverse(schur)
    b21 = -dot3(y, g, ((1,), (0,)))
    b11 = x11 - dot3(g, b21, ((0,), (0,)))
    for i in range(count):
        pack_into(out.at[i], b11[i], b21[i], y[i])


def spread_kernel(n, sections, nhalf, nown, packed, full, rows_out, landed, near_s, near_r, pair_s, side_s, side_r):
    chips = n // 2
    share = BLK // n
    me = lax.axis_index("dp")
    section = lax.axis_index("pipe")
    core = lax.rem(me, 2)
    chip = me // 2
    pair = me + 1 - 2 * core

    barrier = pltpu.get_barrier_semaphore()
    pl.semaphore_signal(barrier, inc=1, device_id={"dp": pair}, device_id_type=MESH)
    for step in range(1, chips):
        other = lax.rem(chip + step, chips) * 2 + core
        pl.semaphore_signal(barrier, inc=1, device_id={"dp": other}, device_id_type=MESH)
    for step in range(1, sections):
        pl.semaphore_signal(
            barrier, inc=1, device_id={"pipe": lax.rem(section + step, sections)}, device_id_type=MESH
        )
    pl.semaphore_wait(barrier, chips + sections - 1)

    def send(source, block, target, sem):
        return pltpu.make_async_remote_copy(
            src_ref=source, dst_ref=landed.at[block], send_sem=sem, recv_sem=near_r.at[block],
            device_id={"dp": target}, device_id_type=MESH,
        )

    def side(block, step):
        mine = full.at[block, pl.ds(pl.multiple_of(me * share, share), share), :]
        return pltpu.make_async_remote_copy(
            src_ref=mine, dst_ref=rows_out.at[section, block], send_sem=side_s.at[block, step - 1],
            recv_sem=side_r.at[section, block],
            device_id={"pipe": lax.rem(section + step, sections)}, device_id_type=MESH,
        )

    def open_block(value, block):
        m11, m21, m22 = unpack(value)
        full[block, 0:HALF, 0:HALF] = m11
        full[block, HALF:BLK, 0:HALF] = m21
        full[block, 0:HALF, HALF:BLK] = m21.T
        full[block, HALF:BLK, HALF:BLK] = m22
        for step in range(1, sections):
            side(block, step).start()
        rows_out[section, block] = full[block, pl.ds(pl.multiple_of(me * share, share), share), :]

    for slot in range(nown):
        t = slot * chips + chip

        @pl.when(t < nhalf)
        def _():
            for step in range(1, chips):
                send(packed.at[slot], 2 * t + core, lax.rem(chip + step, chips) * 2 + core, near_s.at[slot, step - 1]).start()
            send(packed.at[slot], 2 * t + core, pair, pair_s.at[t]).start()

    for slot in range(nown):
        t = slot * chips + chip

        @pl.when(t < nhalf)
        def _():
            open_block(packed[slot], 2 * t + core)

    def arrived(block):
        send(landed.at[block], block, pair, pair_s.at[0]).wait_recv()

    for t in range(nhalf):
        @pl.when(chip != t % chips)
        def _():
            block = 2 * t + core
            arrived(block)
            send(landed.at[block], block, pair, pair_s.at[t]).start()
            open_block(landed[block], block)

        block = 2 * t + 1 - core
        arrived(block)
        open_block(landed[block], block)

    for slot in range(nown):
        t = slot * chips + chip

        @pl.when(t < nhalf)
        def _():
            for step in range(1, chips):
                send(packed.at[slot], 2 * t + core, lax.rem(chip + step, chips) * 2 + core, near_s.at[slot, step - 1]).wait_send()

    for t in range(nhalf):
        send(landed.at[2 * t + core], 2 * t + core, pair, pair_s.at[t]).wait_send()

    @pl.loop(0, 2 * nhalf)
    def _(block):
        for step in range(1, sections):
            side(block, step).wait_send()
            source = lax.rem(section + step, sections)
            pltpu.make_async_remote_copy(
                src_ref=rows_out.at[source, block], dst_ref=rows_out.at[source, block],
                send_sem=side_s.at[block, step - 1], recv_sem=side_r.at[source, block],
                device_id={"pipe": source}, device_id_type=MESH,
            ).wait_recv()


def apply_kernel(per_step, owners, inverse, grad, rows, precond, held, slots):
    step = pl.program_id(0)
    section = lax.axis_index("pipe")
    sections, nblocks = owners.shape
    total = sections * nblocks

    @pl.when(step == 0)
    def _():
        for j in range(HOST):
            slots[j] = -1

        def place(k, used):
            hit = owners[k // nblocks, lax.rem(k, nblocks)] == section

            @pl.when(hit)
            def _():
                slots[used] = k

            return used + hit.astype(jnp.int32)

        lax.fori_loop(0, total, place, jnp.int32(0))

    for j in range(per_step):
        k = slots[step * per_step + j]
        at = jnp.maximum(k, 0)
        value = rows[at // nblocks, lax.rem(at, nblocks)]
        held[j] = jnp.where(k >= 0, value, 0.0)

    a = inverse[0]
    b = grad[...]
    a_high = a.astype(BF16)
    a_low = (a - a_high.astype(F32)).astype(BF16)
    b_high = b.astype(BF16)
    b_low = (b - b_high.astype(F32)).astype(BF16)
    small = jnp.dot(a_high, b_low, preferred_element_type=F32) + jnp.dot(a_low, b_high, preferred_element_type=F32)
    precond[...] = jnp.dot(a_high, b_high, preferred_element_type=F32) + small


def shards(acts, grad, owner_of):
    tokens, feature_count = acts.shape[1:]
    columns = grad.shape[1]
    nblocks = feature_count // BLK
    n = lax.axis_size("dp")
    sections = lax.axis_size("pipe")
    chips = n // 2
    nhalf = nblocks // 2
    nown = -(-nhalf // chips)
    share = BLK // n
    vmem = pl.BlockSpec(memory_space=pltpu.VMEM)
    dma = pltpu.SemaphoreType.DMA
    limit = 56 * 1024 * 1024

    summed = pl.pallas_call(
        functools.partial(reduce_kernel, n, nhalf, nown),
        out_shape=jax.ShapeDtypeStruct((nown, PACK, BLK), F32),
        in_specs=[vmem],
        out_specs=vmem,
        scratch_shapes=[
            pltpu.VMEM((nhalf, PACK, BLK), F32),
            pltpu.VMEM((nhalf, PACK, BLK), F32),
            pltpu.VMEM((nhalf, PACK, BLK), F32),
            pltpu.VMEM((nown, chips, PACK, BLK), F32),
            dma((nhalf,)), dma((nhalf,)), dma((nhalf,)), dma((nown, chips)),
        ],
        compiler_params=pltpu.CompilerParams(collective_id=0, has_side_effects=True),
        name="reduce_factors",
    )(acts[0])

    packed = pl.pallas_call(
        functools.partial(invert_kernel, float(tokens * n)),
        out_shape=jax.ShapeDtypeStruct((nown, PACK, BLK), F32),
        in_specs=[vmem],
        out_specs=vmem,
        name="invert_blocks",
    )(summed)

    inverse, rows = pl.pallas_call(
        functools.partial(spread_kernel, n, sections, nhalf, nown),
        out_shape=(
            jax.ShapeDtypeStruct((nblocks, BLK, BLK), F32),
            jax.ShapeDtypeStruct((sections, nblocks, share, BLK), F32),
        ),
        in_specs=[vmem],
        out_specs=(vmem, vmem),
        scratch_shapes=[
            pltpu.VMEM((nblocks, PACK, BLK), F32),
            dma((nown, chips - 1)), dma((nblocks,)), dma((nhalf,)),
            dma((nblocks, sections - 1)), dma((sections, nblocks)),
        ],
        compiler_params=pltpu.CompilerParams(collective_id=1, has_side_effects=True),
        name="spread_inverses",
    )(packed)

    per_step = HOST // nblocks
    precond, held = pl.pallas_call(
        functools.partial(apply_kernel, per_step),
        grid_spec=pltpu.PrefetchScalarGridSpec(
            num_scalar_prefetch=1,
            grid=(nblocks,),
            in_specs=[
                pl.BlockSpec((1, BLK, BLK), lambda i, o: (i, 0, 0)),
                pl.BlockSpec((BLK, columns), lambda i, o: (i, 0)),
                pl.BlockSpec((sections, nblocks, share, BLK), lambda i, o: (0, 0, 0, 0), pipeline_mode=pl.Buffered(1)),
            ],
            out_specs=[
                pl.BlockSpec((BLK, columns), lambda i, o: (i, 0)),
                pl.BlockSpec((per_step, share, BLK), lambda i, o: (i, 0, 0)),
            ],
            scratch_shapes=[pltpu.SMEM((HOST,), jnp.int32)],
        ),
        out_shape=(
            jax.ShapeDtypeStruct((feature_count, columns), F32),
            jax.ShapeDtypeStruct((HOST, share, BLK), F32),
        ),
        compiler_params=pltpu.CompilerParams(dimension_semantics=("arbitrary",)),
        name="apply_inverses",
    )(owner_of, inverse, grad, rows)
    return precond, held[None]


def solution(mesh):
    placed = (P("pipe", "dp", None), P("pipe", "dp"), P())
    return jax.shard_map(
        shards,
        mesh=mesh,
        in_specs=placed,
        out_specs=(P("pipe", "dp"), P("pipe", None, "dp", None)),
        check_vma=False,
    )
```

```python
import functools

import jax
import jax.numpy as jnp
from jax import lax
from jax.experimental import pallas as pl
from jax.experimental.pallas import tpu as pltpu
from jax.sharding import PartitionSpec as P

BLK = 256
HALF = BLK // 2
PACK = HALF + 8
HOST = 24
MESH = pl.DeviceIdType.MESH

damping_ratio = 0.1
F32 = jnp.float32
BF16 = jnp.bfloat16
HIGHEST = lax.Precision.HIGHEST


def square_iota():
    rows = lax.broadcasted_iota(jnp.int32, (HALF, HALF), 0)
    cols = lax.broadcasted_iota(jnp.int32, (HALF, HALF), 1)
    return rows, cols


def pack_into(ref, m11, m21, m22):
    rows, cols = square_iota()
    diag = jnp.sum(jnp.where(rows == cols, m22, 0.0), axis=0, keepdims=True)
    ref[0:HALF, 0:HALF] = m21
    ref[0:HALF, HALF:BLK] = jnp.where(rows >= cols, m11, m22)
    ref[HALF:PACK, 0:HALF] = jnp.broadcast_to(diag, (PACK - HALF, HALF))
    ref[HALF:PACK, HALF:BLK] = jnp.zeros((PACK - HALF, HALF), F32)


def unpack(value):
    rows, cols = square_iota()
    m21 = value[0:HALF, 0:HALF]
    mixed = value[0:HALF, HALF:BLK]
    diag = value[HALF : HALF + 1, 0:HALF]
    turned = mixed.T
    m11 = jnp.where(rows >= cols, mixed, turned)
    m22 = jnp.where(rows < cols, mixed, jnp.where(rows == cols, diag, turned))
    return m11, m21, m22


def owner_plan(chips, nhalf):
    order = []
    for i in range((chips + 1) // 2):
        order.extend([i] if i == chips - 1 - i else [i, chips - 1 - i])
    return [order[t % chips] for t in range(nhalf)], [order.index(i) for i in range(chips)]


def look_up(table, index):
    return sum((index == i).astype(jnp.int32) * value for i, value in enumerate(table))


def greet(signals):
    barrier = pltpu.get_barrier_semaphore()
    for condition, device in signals:
        if condition is None:
            pl.semaphore_signal(barrier, inc=1, device_id=device, device_id_type=MESH)
        else:
            @pl.when(condition)
            def _():
                pl.semaphore_signal(barrier, inc=1, device_id=device, device_id_type=MESH)
    peers = sum(1 if condition is None else condition.astype(jnp.int32) for condition, _ in signals)
    pl.semaphore_wait(barrier, peers)


def reduce_kernel(n, nhalf, nown, acts, out, theirs, mine, from_pair, from_low, from_high,
                  pair_s, pair_r, line_s, low_r, high_r):
    chips = n // 2
    me = lax.axis_index("dp")
    core = lax.rem(me, 2)
    chip = me // 2
    pair = me + 1 - 2 * core
    low = (jnp.maximum(chip - 1, 0)) * 2 + core
    high = (jnp.minimum(chip + 1, chips - 1)) * 2 + core
    owners, places = owner_plan(chips, nhalf)

    greet([(None, {"dp": pair}), (chip > 0, {"dp": low}), (chip < chips - 1, {"dp": high})])

    def partial(block, ref):
        start = pl.multiple_of(block * BLK, BLK)
        x = acts[:, pl.ds(start, BLK)]
        full = lax.dot_general(x, x, (((0,), (0,)), ((), ())), preferred_element_type=F32)
        pack_into(ref, full[0:HALF, 0:HALF], full[HALF:BLK, 0:HALF], full[HALF:BLK, HALF:BLK])

    def pair_copy(t):
        return pltpu.make_async_remote_copy(
            src_ref=theirs.at[t], dst_ref=from_pair.at[t], send_sem=pair_s.at[t], recv_sem=pair_r.at[t],
            device_id={"dp": pair}, device_id_type=MESH,
        )

    @pl.loop(0, nhalf)
    def _(t):
        partial(2 * t + 1 - core, theirs.at[t])
        pair_copy(t).start()

    @pl.loop(0, nhalf)
    def _(t):
        partial(2 * t + core, mine.at[t])

    @pl.loop(0, nhalf)
    def _(t):
        pair_copy(t).wait()
        mine[t] = mine[t] + from_pair[t]

    def upward(t):
        return pltpu.make_async_remote_copy(
            src_ref=mine.at[t], dst_ref=from_low.at[t], send_sem=line_s.at[t], recv_sem=low_r.at[t],
            device_id={"dp": high}, device_id_type=MESH,
        )

    def downward(t):
        return pltpu.make_async_remote_copy(
            src_ref=mine.at[t], dst_ref=from_high.at[t], send_sem=line_s.at[t], recv_sem=high_r.at[t],
            device_id={"dp": low}, device_id_type=MESH,
        )

    up = sorted((t for t in range(nhalf) if owners[t] > 0), key=lambda t: -owners[t])
    down = sorted((t for t in range(nhalf) if owners[t] < chips - 1), key=lambda t: owners[t])

    @pl.loop(0, nhalf + chips - 1)
    def _(tick):
        i = tick - chip
        t = look_up(up, i)

        @pl.when((i >= 0) & (i < len(up)) & (look_up(owners, t) > chip))
        def _():
            @pl.when(chip > 0)
            def _():
                upward(t).wait_recv()
                mine[t] = mine[t] + from_low[t]

            upward(t).start()

        j = tick - (chips - 1 - chip)
        u = look_up(down, j)

        @pl.when((j >= 0) & (j < len(down)) & (look_up(owners, u) < chip))
        def _():
            @pl.when(chip < chips - 1)
            def _():
                downward(u).wait_recv()
                mine[u] = mine[u] + from_high[u]

            downward(u).start()

    place = look_up(places, chip)
    for slot in range(nown):
        t = slot * chips + place

        @pl.when(t < nhalf)
        def _():
            out[slot] = mine[t]

            @pl.when(chip > 0)
            def _():
                upward(t).wait_recv()
                out[slot] = out[slot] + from_low[t]

            @pl.when(chip < chips - 1)
            def _():
                downward(t).wait_recv()
                out[slot] = out[slot] + from_high[t]

        @pl.when(t >= nhalf)
        def _():
            rows, cols = square_iota()
            eye = jnp.where(rows == cols, 1.0, 0.0)
            pack_into(out.at[slot], eye, jnp.zeros((HALF, HALF), F32), eye)

    for t in range(nhalf):
        @pl.when(chip != owners[t])
        def _():
            upward(t).wait_send()


def dot3(a, b, contract):
    return jnp.stack([
        lax.dot_general(a[i], b[i], (contract, ((), ())), precision=HIGHEST, preferred_element_type=F32)
        for i in range(a.shape[0])
    ])


def sweep_inverse(a):
    count = a.shape[0]
    panel_shape = (count, 8, HALF)
    sub = lax.broadcasted_iota(jnp.int32, panel_shape, 1)
    lane = lax.broadcasted_iota(jnp.int32, panel_shape, 2)
    all_lanes = lax.broadcasted_iota(jnp.int32, (count, HALF, HALF), 2)

    def panel(_, a):
        top = a[:, 0:8, :]
        cols = [jnp.broadcast_to(top[:, :, k : k + 1], panel_shape) for k in range(8)]
        lead = [jnp.broadcast_to(a[:, :, k : k + 1], a.shape) for k in range(8)]
        for k in range(8):
            here = cols[k]
            inv = jnp.broadcast_to(1.0 / here[:, k : k + 1, :], panel_shape)
            row = jnp.broadcast_to(top[:, k : k + 1, :], panel_shape) * inv
            at_row = sub == k
            new = jnp.where(at_row, row, top - here * row)
            edge = jnp.where(at_row, inv, -here * inv)
            top = jnp.where(lane == k, edge, new)
            for j in range(k + 1, 8):
                across = jnp.broadcast_to(cols[j][:, k : k + 1, :], panel_shape) * inv
                cols[j] = jnp.where(at_row, across, cols[j] - here * across)
        top = jnp.where(lane < 8, -top, top)
        rest = a
        for k in range(8):
            rest = rest - lead[k] * top[:, k : k + 1, :]
        tall = jnp.concatenate([top, jnp.zeros((count, HALF - 8, HALF), F32)], axis=1)
        turned = jnp.stack([tall[i].T for i in range(count)])
        rest = jnp.where(all_lanes < 8, turned, rest)
        a = jnp.concatenate([rest[:, 8:, :], top], axis=1)
        return pltpu.roll(a, HALF - 8, 2)

    return -lax.fori_loop(0, HALF // 8, panel, a)


def invert_kernel(tokens, packed, out):
    count = packed.shape[0]
    rows, cols = square_iota()
    parts = [unpack(packed[i] / tokens) for i in range(count)]
    m11 = jnp.stack([p[0] for p in parts])
    m21 = jnp.stack([p[1] for p in parts])
    m22 = jnp.stack([p[2] for p in parts])
    eye = rows == cols
    trace = jnp.sum(jnp.where(eye, m11 + m22, 0.0), axis=(1, 2), keepdims=True)
    damping = jnp.where(eye, damping_ratio * trace / BLK, 0.0)
    x11 = sweep_inverse(m11 + damping)
    g = dot3(m21, x11, ((1,), (0,)))
    schur = m22 + damping - dot3(g, m21, ((1,), (1,)))
    y = sweep_inverse(schur)
    b21 = -dot3(y, g, ((1,), (0,)))
    b11 = x11 - dot3(g, b21, ((0,), (0,)))
    for i in range(count):
        pack_into(out.at[i], b11[i], b21[i], y[i])


def spread_kernel(n, sections, nhalf, nown, packed, full, rows_out, landed, low_s, high_s, near_r, pair_s, side_s, side_r):
    chips = n // 2
    share = BLK // n
    me = lax.axis_index("dp")
    section = lax.axis_index("pipe")
    core = lax.rem(me, 2)
    chip = me // 2
    pair = me + 1 - 2 * core
    low = (jnp.maximum(chip - 1, 0)) * 2 + core
    high = (jnp.minimum(chip + 1, chips - 1)) * 2 + core
    owners, places = owner_plan(chips, nhalf)

    greet(
        [(None, {"dp": pair}), (chip > 0, {"dp": low}), (chip < chips - 1, {"dp": high})]
        + [(None, {"pipe": lax.rem(section + step, sections)}) for step in range(1, sections)]
    )

    def send(source, t, half, target, sem):
        block = 2 * t + half
        return pltpu.make_async_remote_copy(
            src_ref=source, dst_ref=landed.at[block], send_sem=sem.at[t], recv_sem=near_r.at[block],
            device_id={"dp": target}, device_id_type=MESH,
        )

    def side(block, step):
        mine = full.at[block, pl.ds(pl.multiple_of(me * share, share), share), :]
        return pltpu.make_async_remote_copy(
            src_ref=mine, dst_ref=rows_out.at[section, block], send_sem=side_s.at[block, step - 1],
            recv_sem=side_r.at[section, block],
            device_id={"pipe": lax.rem(section + step, sections)}, device_id_type=MESH,
        )

    def open_block(value, block):
        m11, m21, m22 = unpack(value)
        full[block, 0:HALF, 0:HALF] = m11
        full[block, HALF:BLK, 0:HALF] = m21
        full[block, 0:HALF, HALF:BLK] = m21.T
        full[block, HALF:BLK, HALF:BLK] = m22
        for step in range(1, sections):
            side(block, step).start()
        rows_out[section, block] = full[block, pl.ds(pl.multiple_of(me * share, share), share), :]

    place = look_up(places, chip)
    for slot in range(nown):
        t = slot * chips + place

        @pl.when(t < nhalf)
        def _():
            @pl.when(chip > 0)
            def _():
                send(packed.at[slot], t, core, low, low_s).start()

            @pl.when(chip < chips - 1)
            def _():
                send(packed.at[slot], t, core, high, high_s).start()

            send(packed.at[slot], t, core, pair, pair_s).start()

    def arrived(t, half):
        send(landed.at[2 * t + half], t, half, pair, pair_s).wait_recv()

    def receive(t):
        arrived(t, core)
        source = landed.at[2 * t + core]

        @pl.when((look_up(owners, t) > chip) & (chip > 0))
        def _():
            send(source, t, core, low, low_s).start()

        @pl.when((look_up(owners, t) < chip) & (chip < chips - 1))
        def _():
            send(source, t, core, high, high_s).start()

        send(source, t, core, pair, pair_s).start()

    for slot in range(nown):
        t = slot * chips + place

        @pl.when(t < nhalf)
        def _():
            open_block(packed[slot], 2 * t + core)
            other = 2 * t + 1 - core
            arrived(t, 1 - core)
            open_block(landed[other], other)

    from_high = sorted(range(nhalf), key=lambda t: owners[t])
    from_low = sorted(range(nhalf), key=lambda t: -owners[t])
    below = sum((chip >= owner).astype(jnp.int32) for owner in owners)
    above = sum((chip <= owner).astype(jnp.int32) for owner in owners)

    @pl.loop(0, nhalf)
    def _(tick):
        i = tick + below
        t = look_up(from_high, i)
        j = tick + above
        u = look_up(from_low, j)

        @pl.when(i < nhalf)
        def _():
            receive(t)

        @pl.when(j < nhalf)
        def _():
            receive(u)

        for half in (core, 1 - core):
            for use, which in ((i < nhalf, t), (j < nhalf, u)):
                @pl.when(use)
                def _():
                    block = 2 * which + half
                    if half is not core:
                        arrived(which, half)
                    open_block(landed[block], block)

    for t in range(nhalf):
        owner = owners[t]
        source = landed.at[2 * t + core]

        @pl.when((chip > 0) & (chip <= owner))
        def _():
            send(source, t, core, low, low_s).wait_send()

        @pl.when((chip < chips - 1) & (chip >= owner))
        def _():
            send(source, t, core, high, high_s).wait_send()

        send(source, t, core, pair, pair_s).wait_send()

    @pl.loop(0, 2 * nhalf)
    def _(block):
        for step in range(1, sections):
            side(block, step).wait_send()
            source = lax.rem(section + step, sections)
            pltpu.make_async_remote_copy(
                src_ref=rows_out.at[source, block], dst_ref=rows_out.at[source, block],
                send_sem=side_s.at[block, step - 1], recv_sem=side_r.at[source, block],
                device_id={"pipe": source}, device_id_type=MESH,
            ).wait_recv()


def apply_kernel(per_step, owners, inverse, grad, rows, precond, held, slots):
    step = pl.program_id(0)
    section = lax.axis_index("pipe")
    sections, nblocks = owners.shape
    total = sections * nblocks

    @pl.when(step == 0)
    def _():
        for j in range(HOST):
            slots[j] = -1

        def place(k, used):
            hit = owners[k // nblocks, lax.rem(k, nblocks)] == section

            @pl.when(hit)
            def _():
                slots[used] = k

            return used + hit.astype(jnp.int32)

        lax.fori_loop(0, total, place, jnp.int32(0))

    for j in range(per_step):
        k = slots[step * per_step + j]
        at = jnp.maximum(k, 0)
        value = rows[at // nblocks, lax.rem(at, nblocks)]
        held[j] = jnp.where(k >= 0, value, 0.0)

    for i in range(inverse.shape[0]):
        span = slice(i * BLK, (i + 1) * BLK)
        a = inverse[i]
        b = grad[span, :]
        a_high = a.astype(BF16)
        a_low = (a - a_high.astype(F32)).astype(BF16)
        b_high = b.astype(BF16)
        b_low = (b - b_high.astype(F32)).astype(BF16)
        small = jnp.dot(a_high, b_low, preferred_element_type=F32) + jnp.dot(a_low, b_high, preferred_element_type=F32)
        precond[span, :] = jnp.dot(a_high, b_high, preferred_element_type=F32) + small


def shards(acts, grad, owner_of):
    tokens, feature_count = acts.shape[1:]
    columns = grad.shape[1]
    nblocks = feature_count // BLK
    n = lax.axis_size("dp")
    sections = lax.axis_size("pipe")
    chips = n // 2
    nhalf = nblocks // 2
    nown = -(-nhalf // chips)
    share = BLK // n
    vmem = pl.BlockSpec(memory_space=pltpu.VMEM)
    dma = pltpu.SemaphoreType.DMA

    summed = pl.pallas_call(
        functools.partial(reduce_kernel, n, nhalf, nown),
        out_shape=jax.ShapeDtypeStruct((nown, PACK, BLK), F32),
        in_specs=[vmem],
        out_specs=vmem,
        scratch_shapes=[
            pltpu.VMEM((nhalf, PACK, BLK), F32),
            pltpu.VMEM((nhalf, PACK, BLK), F32),
            pltpu.VMEM((nhalf, PACK, BLK), F32),
            pltpu.VMEM((nhalf, PACK, BLK), F32),
            pltpu.VMEM((nhalf, PACK, BLK), F32),
            dma((nhalf,)), dma((nhalf,)), dma((nhalf,)), dma((nhalf,)), dma((nhalf,)),
        ],
        compiler_params=pltpu.CompilerParams(collective_id=0, has_side_effects=True),
        name="reduce_factors",
    )(acts[0])

    packed = pl.pallas_call(
        functools.partial(invert_kernel, float(tokens * n)),
        out_shape=jax.ShapeDtypeStruct((nown, PACK, BLK), F32),
        in_specs=[vmem],
        out_specs=vmem,
        name="invert_blocks",
    )(summed)

    inverse, rows = pl.pallas_call(
        functools.partial(spread_kernel, n, sections, nhalf, nown),
        out_shape=(
            jax.ShapeDtypeStruct((nblocks, BLK, BLK), F32),
            jax.ShapeDtypeStruct((sections, nblocks, share, BLK), F32),
        ),
        in_specs=[vmem],
        out_specs=(vmem, vmem),
        scratch_shapes=[
            pltpu.VMEM((nblocks, PACK, BLK), F32),
            dma((nhalf,)), dma((nhalf,)), dma((nblocks,)), dma((nhalf,)),
            dma((nblocks, sections - 1)), dma((sections, nblocks)),
        ],
        compiler_params=pltpu.CompilerParams(collective_id=1, has_side_effects=True),
        name="spread_inverses",
    )(packed)

    group = 2 if nblocks % 2 == 0 else 1
    per_step = HOST // (nblocks // group)
    precond, held = pl.pallas_call(
        functools.partial(apply_kernel, per_step),
        grid_spec=pltpu.PrefetchScalarGridSpec(
            num_scalar_prefetch=1,
            grid=(nblocks // group,),
            in_specs=[
                pl.BlockSpec((group, BLK, BLK), lambda i, o: (i, 0, 0)),
                pl.BlockSpec((group * BLK, columns), lambda i, o: (i, 0)),
                pl.BlockSpec((sections, nblocks, share, BLK), lambda i, o: (0, 0, 0, 0), pipeline_mode=pl.Buffered(1)),
            ],
            out_specs=[
                pl.BlockSpec((group * BLK, columns), lambda i, o: (i, 0)),
                pl.BlockSpec((per_step, share, BLK), lambda i, o: (i, 0, 0)),
            ],
            scratch_shapes=[pltpu.SMEM((HOST,), jnp.int32)],
        ),
        out_shape=(
            jax.ShapeDtypeStruct((feature_count, columns), F32),
            jax.ShapeDtypeStruct((HOST, share, BLK), F32),
        ),
        compiler_params=pltpu.CompilerParams(dimension_semantics=("arbitrary",)),
        name="apply_inverses",
    )(owner_of, inverse, grad, rows)
    return precond, held[None]


def solution(mesh):
    placed = (P("pipe", "dp", None), P("pipe", "dp"), P())
    return jax.shard_map(
        shards,
        mesh=mesh,
        in_specs=placed,
        out_specs=(P("pipe", "dp"), P("pipe", None, "dp", None)),
        check_vma=False,
    )
```

```python
import functools

import jax
import jax.numpy as jnp
from jax import lax
from jax.experimental import pallas as pl
from jax.experimental.pallas import tpu as pltpu
from jax.sharding import PartitionSpec as P

BLK = 256
HALF = BLK // 2
PACK = HALF + 8
HOST = 24
UNROLL = 1
MESH = pl.DeviceIdType.MESH

damping_ratio = 0.1
F32 = jnp.float32
BF16 = jnp.bfloat16
HIGHEST = lax.Precision.HIGHEST


def square_iota():
    rows = lax.broadcasted_iota(jnp.int32, (HALF, HALF), 0)
    cols = lax.broadcasted_iota(jnp.int32, (HALF, HALF), 1)
    return rows, cols


def pack_into(ref, m11, m21, m22):
    rows, cols = square_iota()
    diag = jnp.sum(jnp.where(rows == cols, m22, 0.0), axis=0, keepdims=True)
    ref[0:HALF, 0:HALF] = m21
    ref[0:HALF, HALF:BLK] = jnp.where(rows >= cols, m11, m22)
    ref[HALF:PACK, 0:HALF] = jnp.broadcast_to(diag, (PACK - HALF, HALF))
    ref[HALF:PACK, HALF:BLK] = jnp.zeros((PACK - HALF, HALF), F32)


def unpack(value):
    rows, cols = square_iota()
    m21 = value[0:HALF, 0:HALF]
    mixed = value[0:HALF, HALF:BLK]
    diag = value[HALF : HALF + 1, 0:HALF]
    turned = mixed.T
    m11 = jnp.where(rows >= cols, mixed, turned)
    m22 = jnp.where(rows < cols, mixed, jnp.where(rows == cols, diag, turned))
    return m11, m21, m22


def owner_plan(chips, nhalf):
    order = []
    for i in range((chips + 1) // 2):
        order.extend([i] if i == chips - 1 - i else [i, chips - 1 - i])
    return [order[t % chips] for t in range(nhalf)], [order.index(i) for i in range(chips)]


def look_up(table, index):
    return sum((index == i).astype(jnp.int32) * value for i, value in enumerate(table))


def greet(signals):
    barrier = pltpu.get_barrier_semaphore()
    for condition, device in signals:
        if condition is None:
            pl.semaphore_signal(barrier, inc=1, device_id=device, device_id_type=MESH)
        else:
            @pl.when(condition)
            def _():
                pl.semaphore_signal(barrier, inc=1, device_id=device, device_id_type=MESH)
    peers = sum(1 if condition is None else condition.astype(jnp.int32) for condition, _ in signals)
    pl.semaphore_wait(barrier, peers)


def reduce_kernel(n, nhalf, nown, acts, out, theirs, mine, from_pair, from_low, from_high,
                  pair_s, pair_r, line_s, low_r, high_r):
    chips = n // 2
    me = lax.axis_index("dp")
    core = lax.rem(me, 2)
    chip = me // 2
    pair = me + 1 - 2 * core
    low = (jnp.maximum(chip - 1, 0)) * 2 + core
    high = (jnp.minimum(chip + 1, chips - 1)) * 2 + core
    owners, places = owner_plan(chips, nhalf)

    greet([(None, {"dp": pair}), (chip > 0, {"dp": low}), (chip < chips - 1, {"dp": high})])

    def partial(block, ref):
        start = pl.multiple_of(block * BLK, BLK)
        x = acts[:, pl.ds(start, BLK)]
        full = lax.dot_general(x, x, (((0,), (0,)), ((), ())), preferred_element_type=F32)
        pack_into(ref, full[0:HALF, 0:HALF], full[HALF:BLK, 0:HALF], full[HALF:BLK, HALF:BLK])

    def pair_copy(t):
        return pltpu.make_async_remote_copy(
            src_ref=theirs.at[t], dst_ref=from_pair.at[t], send_sem=pair_s.at[t], recv_sem=pair_r.at[t],
            device_id={"dp": pair}, device_id_type=MESH,
        )

    def fold_pair(t):
        pair_copy(t).wait()
        mine[t] = mine[t] + from_pair[t]

    def upward(t):
        return pltpu.make_async_remote_copy(
            src_ref=mine.at[t], dst_ref=from_low.at[t], send_sem=line_s.at[t], recv_sem=low_r.at[t],
            device_id={"dp": high}, device_id_type=MESH,
        )

    def downward(t):
        return pltpu.make_async_remote_copy(
            src_ref=mine.at[t], dst_ref=from_high.at[t], send_sem=line_s.at[t], recv_sem=high_r.at[t],
            device_id={"dp": low}, device_id_type=MESH,
        )

    up = sorted((t for t in range(nhalf) if owners[t] > 0), key=lambda t: -owners[t])
    down = sorted((t for t in range(nhalf) if owners[t] < chips - 1), key=lambda t: owners[t])

    turns = sorted(range(nhalf), key=lambda t: (min(up.index(t) if t in up else nhalf, down.index(t) if t in down else nhalf), t))

    @pl.loop(0, nhalf + chips)
    def _(tick):
        for turn in (2 * tick, 2 * tick + 1):
            @pl.when(turn < nhalf)
            def _():
                t = look_up(turns, turn)
                partial(2 * t + 1 - core, theirs.at[t])
                pair_copy(t).start()
                partial(2 * t + core, mine.at[t])

        i = tick - 1 - chip
        t = look_up(up, i)

        @pl.when((i >= 0) & (i < len(up)) & (look_up(owners, t) > chip))
        def _():
            fold_pair(t)

            @pl.when(chip > 0)
            def _():
                upward(t).wait_recv()
                mine[t] = mine[t] + from_low[t]

            upward(t).start()

        j = tick - 1 - (chips - 1 - chip)
        u = look_up(down, j)

        @pl.when((j >= 0) & (j < len(down)) & (look_up(owners, u) < chip))
        def _():
            fold_pair(u)

            @pl.when(chip < chips - 1)
            def _():
                downward(u).wait_recv()
                mine[u] = mine[u] + from_high[u]

            downward(u).start()

    place = look_up(places, chip)
    for slot in range(nown):
        t = slot * chips + place

        @pl.when(t < nhalf)
        def _():
            fold_pair(t)
            out[slot] = mine[t]

            @pl.when(chip > 0)
            def _():
                upward(t).wait_recv()
                out[slot] = out[slot] + from_low[t]

            @pl.when(chip < chips - 1)
            def _():
                downward(t).wait_recv()
                out[slot] = out[slot] + from_high[t]

        @pl.when(t >= nhalf)
        def _():
            rows, cols = square_iota()
            eye = jnp.where(rows == cols, 1.0, 0.0)
            pack_into(out.at[slot], eye, jnp.zeros((HALF, HALF), F32), eye)

    for t in range(nhalf):
        @pl.when(chip != owners[t])
        def _():
            upward(t).wait_send()


def dot3(a, b, contract):
    return jnp.stack([
        lax.dot_general(a[i], b[i], (contract, ((), ())), precision=HIGHEST, preferred_element_type=F32)
        for i in range(a.shape[0])
    ])


def sweep_inverse(a):
    count = a.shape[0]
    panel_shape = (count, 8, HALF)
    sub = lax.broadcasted_iota(jnp.int32, panel_shape, 1)
    lane = lax.broadcasted_iota(jnp.int32, panel_shape, 2)
    all_lanes = lax.broadcasted_iota(jnp.int32, (count, HALF, HALF), 2)

    def columns_of(top, first):
        return tuple(jnp.broadcast_to(top[:, :, k : k + 1], panel_shape) for k in range(first, first + 8))

    def panel(_, state):
        a, cols = state
        cols = list(cols)
        top = a[:, 0:8, :]
        for k in range(8):
            here = cols[k]
            inv = jnp.broadcast_to(1.0 / here[:, k : k + 1, :], panel_shape)
            row = jnp.broadcast_to(top[:, k : k + 1, :], panel_shape) * inv
            at_row = sub == k
            new = jnp.where(at_row, row, top - here * row)
            edge = jnp.where(at_row, inv, -here * inv)
            top = jnp.where(lane == k, edge, new)
            for j in range(k + 1, 8):
                across = jnp.broadcast_to(cols[j][:, k : k + 1, :], panel_shape) * inv
                cols[j] = jnp.where(at_row, across, cols[j] - here * across)
        top = jnp.where(lane < 8, -top, top)
        rest = a - jnp.stack([
            lax.dot_general(a[i, 0:8, :], top[i], (((0,), (0,)), ((), ())), precision=HIGHEST, preferred_element_type=F32)
            for i in range(count)
        ])
        ahead = columns_of(rest[:, 8:16, :], 8)
        tall = jnp.concatenate([top, jnp.zeros((count, HALF - 8, HALF), F32)], axis=1)
        turned = jnp.stack([tall[i].T for i in range(count)])
        rest = jnp.where(all_lanes < 8, turned, rest)
        a = jnp.concatenate([rest[:, 8:, :], top], axis=1)
        return pltpu.roll(a, HALF - 8, 2), ahead

    return -lax.fori_loop(0, HALF // 8, panel, (a, columns_of(a[:, 0:8, :], 0)), unroll=UNROLL)[0]


def invert_kernel(tokens, packed, out):
    count = packed.shape[0]
    rows, cols = square_iota()
    parts = [unpack(packed[i] / tokens) for i in range(count)]
    m11 = jnp.stack([p[0] for p in parts])
    m21 = jnp.stack([p[1] for p in parts])
    m22 = jnp.stack([p[2] for p in parts])
    eye = rows == cols
    trace = jnp.sum(jnp.where(eye, m11 + m22, 0.0), axis=(1, 2), keepdims=True)
    damping = jnp.where(eye, damping_ratio * trace / BLK, 0.0)
    x11 = sweep_inverse(m11 + damping)
    g = dot3(m21, x11, ((1,), (0,)))
    schur = m22 + damping - dot3(g, m21, ((1,), (1,)))
    y = sweep_inverse(schur)
    b21 = -dot3(y, g, ((1,), (0,)))
    b11 = x11 - dot3(g, b21, ((0,), (0,)))
    for i in range(count):
        pack_into(out.at[i], b11[i], b21[i], y[i])


def spread_kernel(n, sections, nhalf, nown, packed, full, rows_out, landed, low_s, high_s, near_r, pair_s, side_s, side_r):
    chips = n // 2
    share = BLK // n
    me = lax.axis_index("dp")
    section = lax.axis_index("pipe")
    core = lax.rem(me, 2)
    chip = me // 2
    pair = me + 1 - 2 * core
    low = (jnp.maximum(chip - 1, 0)) * 2 + core
    high = (jnp.minimum(chip + 1, chips - 1)) * 2 + core
    owners, places = owner_plan(chips, nhalf)

    greet(
        [(None, {"dp": pair}), (chip > 0, {"dp": low}), (chip < chips - 1, {"dp": high})]
        + [(None, {"pipe": lax.rem(section + step, sections)}) for step in range(1, sections)]
    )

    def send(source, t, half, target, sem):
        block = 2 * t + half
        return pltpu.make_async_remote_copy(
            src_ref=source, dst_ref=landed.at[block], send_sem=sem.at[t], recv_sem=near_r.at[block],
            device_id={"dp": target}, device_id_type=MESH,
        )

    def side(block, step):
        mine = full.at[block, pl.ds(pl.multiple_of(me * share, share), share), :]
        return pltpu.make_async_remote_copy(
            src_ref=mine, dst_ref=rows_out.at[section, block], send_sem=side_s.at[block, step - 1],
            recv_sem=side_r.at[section, block],
            device_id={"pipe": lax.rem(section + step, sections)}, device_id_type=MESH,
        )

    def open_block(value, block):
        m11, m21, m22 = unpack(value)
        full[block, 0:HALF, 0:HALF] = m11
        full[block, HALF:BLK, 0:HALF] = m21
        full[block, 0:HALF, HALF:BLK] = m21.T
        full[block, HALF:BLK, HALF:BLK] = m22
        for step in range(1, sections):
            side(block, step).start()
        rows_out[section, block] = full[block, pl.ds(pl.multiple_of(me * share, share), share), :]

    place = look_up(places, chip)
    for slot in range(nown):
        t = slot * chips + place

        @pl.when(t < nhalf)
        def _():
            @pl.when(chip > 0)
            def _():
                send(packed.at[slot], t, core, low, low_s).start()

            @pl.when(chip < chips - 1)
            def _():
                send(packed.at[slot], t, core, high, high_s).start()

            send(packed.at[slot], t, core, pair, pair_s).start()

    def arrived(t, half):
        send(landed.at[2 * t + half], t, half, pair, pair_s).wait_recv()

    def receive(t):
        arrived(t, core)
        source = landed.at[2 * t + core]

        @pl.when((look_up(owners, t) > chip) & (chip > 0))
        def _():
            send(source, t, core, low, low_s).start()

        @pl.when((look_up(owners, t) < chip) & (chip < chips - 1))
        def _():
            send(source, t, core, high, high_s).start()

        send(source, t, core, pair, pair_s).start()

    for slot in range(nown):
        t = slot * chips + place

        @pl.when(t < nhalf)
        def _():
            open_block(packed[slot], 2 * t + core)
            other = 2 * t + 1 - core
            arrived(t, 1 - core)
            open_block(landed[other], other)

    from_high = sorted(range(nhalf), key=lambda t: owners[t])
    from_low = sorted(range(nhalf), key=lambda t: -owners[t])
    below = sum((chip >= owner).astype(jnp.int32) for owner in owners)
    above = sum((chip <= owner).astype(jnp.int32) for owner in owners)

    @pl.loop(0, nhalf)
    def _(tick):
        i = tick + below
        t = look_up(from_high, i)
        j = tick + above
        u = look_up(from_low, j)

        @pl.when(i < nhalf)
        def _():
            receive(t)

        @pl.when(j < nhalf)
        def _():
            receive(u)

        for half in (core, 1 - core):
            for use, which in ((i < nhalf, t), (j < nhalf, u)):
                @pl.when(use)
                def _():
                    block = 2 * which + half
                    if half is not core:
                        arrived(which, half)
                    open_block(landed[block], block)

    for t in range(nhalf):
        owner = owners[t]
        source = landed.at[2 * t + core]

        @pl.when((chip > 0) & (chip <= owner))
        def _():
            send(source, t, core, low, low_s).wait_send()

        @pl.when((chip < chips - 1) & (chip >= owner))
        def _():
            send(source, t, core, high, high_s).wait_send()

        send(source, t, core, pair, pair_s).wait_send()

    @pl.loop(0, 2 * nhalf)
    def _(block):
        for step in range(1, sections):
            side(block, step).wait_send()
            source = lax.rem(section + step, sections)
            pltpu.make_async_remote_copy(
                src_ref=rows_out.at[source, block], dst_ref=rows_out.at[source, block],
                send_sem=side_s.at[block, step - 1], recv_sem=side_r.at[source, block],
                device_id={"pipe": source}, device_id_type=MESH,
            ).wait_recv()


def apply_kernel(per_step, owners, inverse, grad, rows, precond, held, slots):
    step = pl.program_id(0)
    section = lax.axis_index("pipe")
    sections, nblocks = owners.shape
    total = sections * nblocks

    @pl.when(step == 0)
    def _():
        for j in range(HOST):
            slots[j] = -1

        def place(k, used):
            hit = owners[k // nblocks, lax.rem(k, nblocks)] == section

            @pl.when(hit)
            def _():
                slots[used] = k

            return used + hit.astype(jnp.int32)

        lax.fori_loop(0, total, place, jnp.int32(0))

    for j in range(per_step):
        k = slots[step * per_step + j]
        at = jnp.maximum(k, 0)
        value = rows[at // nblocks, lax.rem(at, nblocks)]
        held[j] = jnp.where(k >= 0, value, 0.0)

    for i in range(inverse.shape[0]):
        span = slice(i * BLK, (i + 1) * BLK)
        a = inverse[i]
        b = grad[span, :]
        a_high = a.astype(BF16)
        a_low = (a - a_high.astype(F32)).astype(BF16)
        b_high = b.astype(BF16)
        b_low = (b - b_high.astype(F32)).astype(BF16)
        small = jnp.dot(a_high, b_low, preferred_element_type=F32) + jnp.dot(a_low, b_high, preferred_element_type=F32)
        precond[span, :] = jnp.dot(a_high, b_high, preferred_element_type=F32) + small


def shards(acts, grad, owner_of):
    tokens, feature_count = acts.shape[1:]
    columns = grad.shape[1]
    nblocks = feature_count // BLK
    n = lax.axis_size("dp")
    sections = lax.axis_size("pipe")
    chips = n // 2
    nhalf = nblocks // 2
    nown = -(-nhalf // chips)
    share = BLK // n
    vmem = pl.BlockSpec(memory_space=pltpu.VMEM)
    dma = pltpu.SemaphoreType.DMA

    summed = pl.pallas_call(
        functools.partial(reduce_kernel, n, nhalf, nown),
        out_shape=jax.ShapeDtypeStruct((nown, PACK, BLK), F32),
        in_specs=[vmem],
        out_specs=vmem,
        scratch_shapes=[
            pltpu.VMEM((nhalf, PACK, BLK), F32),
            pltpu.VMEM((nhalf, PACK, BLK), F32),
            pltpu.VMEM((nhalf, PACK, BLK), F32),
            pltpu.VMEM((nhalf, PACK, BLK), F32),
            pltpu.VMEM((nhalf, PACK, BLK), F32),
            dma((nhalf,)), dma((nhalf,)), dma((nhalf,)), dma((nhalf,)), dma((nhalf,)),
        ],
        compiler_params=pltpu.CompilerParams(collective_id=0, has_side_effects=True),
        name="reduce_factors",
    )(acts[0])

    packed = pl.pallas_call(
        functools.partial(invert_kernel, float(tokens * n)),
        out_shape=jax.ShapeDtypeStruct((nown, PACK, BLK), F32),
        in_specs=[vmem],
        out_specs=vmem,
        name="invert_blocks",
    )(summed)

    inverse, rows = pl.pallas_call(
        functools.partial(spread_kernel, n, sections, nhalf, nown),
        out_shape=(
            jax.ShapeDtypeStruct((nblocks, BLK, BLK), F32),
            jax.ShapeDtypeStruct((sections, nblocks, share, BLK), F32),
        ),
        in_specs=[vmem],
        out_specs=(vmem, vmem),
        scratch_shapes=[
            pltpu.VMEM((nblocks, PACK, BLK), F32),
            dma((nhalf,)), dma((nhalf,)), dma((nblocks,)), dma((nhalf,)),
            dma((nblocks, sections - 1)), dma((sections, nblocks)),
        ],
        compiler_params=pltpu.CompilerParams(collective_id=1, has_side_effects=True),
        name="spread_inverses",
    )(packed)

    group = 2 if nblocks % 2 == 0 else 1
    per_step = HOST // (nblocks // group)
    precond, held = pl.pallas_call(
        functools.partial(apply_kernel, per_step),
        grid_spec=pltpu.PrefetchScalarGridSpec(
            num_scalar_prefetch=1,
            grid=(nblocks // group,),
            in_specs=[
                pl.BlockSpec((group, BLK, BLK), lambda i, o: (i, 0, 0)),
                pl.BlockSpec((group * BLK, columns), lambda i, o: (i, 0)),
                pl.BlockSpec((sections, nblocks, share, BLK), lambda i, o: (0, 0, 0, 0), pipeline_mode=pl.Buffered(1)),
            ],
            out_specs=[
                pl.BlockSpec((group * BLK, columns), lambda i, o: (i, 0)),
                pl.BlockSpec((per_step, share, BLK), lambda i, o: (i, 0, 0)),
            ],
            scratch_shapes=[pltpu.SMEM((HOST,), jnp.int32)],
        ),
        out_shape=(
            jax.ShapeDtypeStruct((feature_count, columns), F32),
            jax.ShapeDtypeStruct((HOST, share, BLK), F32),
        ),
        compiler_params=pltpu.CompilerParams(dimension_semantics=("arbitrary",)),
        name="apply_inverses",
    )(owner_of, inverse, grad, rows)
    return precond, held[None]


def solution(mesh):
    placed = (P("pipe", "dp", None), P("pipe", "dp"), P())
    return jax.shard_map(
        shards,
        mesh=mesh,
        in_specs=placed,
        out_specs=(P("pipe", "dp"), P("pipe", None, "dp", None)),
        check_vma=False,
    )
```

```python
import functools

import jax
import jax.numpy as jnp
from jax import lax
from jax.experimental import pallas as pl
from jax.experimental.pallas import tpu as pltpu
from jax.sharding import PartitionSpec as P

BLK = 256
HALF = BLK // 2
PACK = HALF + 8
HOST = 24
UNROLL = 1
MESH = pl.DeviceIdType.MESH

damping_ratio = 0.1
F32 = jnp.float32
BF16 = jnp.bfloat16
HIGHEST = lax.Precision.HIGHEST


def square_iota():
    rows = lax.broadcasted_iota(jnp.int32, (HALF, HALF), 0)
    cols = lax.broadcasted_iota(jnp.int32, (HALF, HALF), 1)
    return rows, cols


def pack_into(ref, m11, m21, m22):
    rows, cols = square_iota()
    diag = jnp.sum(jnp.where(rows == cols, m22, 0.0), axis=0, keepdims=True)
    ref[0:HALF, 0:HALF] = m21
    ref[0:HALF, HALF:BLK] = jnp.where(rows >= cols, m11, m22)
    ref[HALF:PACK, 0:HALF] = jnp.broadcast_to(diag, (PACK - HALF, HALF))
    ref[HALF:PACK, HALF:BLK] = jnp.zeros((PACK - HALF, HALF), F32)


def unpack(value):
    rows, cols = square_iota()
    m21 = value[0:HALF, 0:HALF]
    mixed = value[0:HALF, HALF:BLK]
    diag = value[HALF : HALF + 1, 0:HALF]
    turned = mixed.T
    m11 = jnp.where(rows >= cols, mixed, turned)
    m22 = jnp.where(rows < cols, mixed, jnp.where(rows == cols, diag, turned))
    return m11, m21, m22


def owner_plan(chips, nhalf):
    order = []
    for i in range((chips + 1) // 2):
        order.extend([i] if i == chips - 1 - i else [i, chips - 1 - i])
    return [order[t % chips] for t in range(nhalf)], [order.index(i) for i in range(chips)]


def look_up(table, index):
    return sum((index == i).astype(jnp.int32) * value for i, value in enumerate(table))


def greet(signals):
    barrier = pltpu.get_barrier_semaphore()
    for condition, device in signals:
        if condition is None:
            pl.semaphore_signal(barrier, inc=1, device_id=device, device_id_type=MESH)
        else:
            @pl.when(condition)
            def _():
                pl.semaphore_signal(barrier, inc=1, device_id=device, device_id_type=MESH)
    peers = sum(1 if condition is None else condition.astype(jnp.int32) for condition, _ in signals)
    pl.semaphore_wait(barrier, peers)


def reduce_kernel(n, nhalf, nown, acts, out, theirs, mine, from_pair, from_low, from_high,
                  pair_s, pair_r, line_s, low_r, high_r):
    chips = n // 2
    me = lax.axis_index("dp")
    core = lax.rem(me, 2)
    chip = me // 2
    pair = me + 1 - 2 * core
    low = (jnp.maximum(chip - 1, 0)) * 2 + core
    high = (jnp.minimum(chip + 1, chips - 1)) * 2 + core
    owners, places = owner_plan(chips, nhalf)

    greet([(None, {"dp": pair}), (chip > 0, {"dp": low}), (chip < chips - 1, {"dp": high})])

    def partial(block, ref):
        start = pl.multiple_of(block * BLK, BLK)
        x = acts[:, pl.ds(start, BLK)]
        full = lax.dot_general(x, x, (((0,), (0,)), ((), ())), preferred_element_type=F32)
        pack_into(ref, full[0:HALF, 0:HALF], full[HALF:BLK, 0:HALF], full[HALF:BLK, HALF:BLK])

    def pair_copy(t):
        return pltpu.make_async_remote_copy(
            src_ref=theirs.at[t], dst_ref=from_pair.at[t], send_sem=pair_s.at[t], recv_sem=pair_r.at[t],
            device_id={"dp": pair}, device_id_type=MESH,
        )

    def fold_pair(t):
        pair_copy(t).wait()
        mine[t] = mine[t] + from_pair[t]

    def upward(t):
        return pltpu.make_async_remote_copy(
            src_ref=mine.at[t], dst_ref=from_low.at[t], send_sem=line_s.at[t], recv_sem=low_r.at[t],
            device_id={"dp": high}, device_id_type=MESH,
        )

    def downward(t):
        return pltpu.make_async_remote_copy(
            src_ref=mine.at[t], dst_ref=from_high.at[t], send_sem=line_s.at[t], recv_sem=high_r.at[t],
            device_id={"dp": low}, device_id_type=MESH,
        )

    up = sorted((t for t in range(nhalf) if owners[t] > 0), key=lambda t: -owners[t])
    down = sorted((t for t in range(nhalf) if owners[t] < chips - 1), key=lambda t: owners[t])

    turns = sorted(range(nhalf), key=lambda t: (min(up.index(t) if t in up else nhalf, down.index(t) if t in down else nhalf), t))

    @pl.loop(0, nhalf + chips)
    def _(tick):
        for turn in (2 * tick, 2 * tick + 1):
            @pl.when(turn < nhalf)
            def _():
                t = look_up(turns, turn)
                partial(2 * t + 1 - core, theirs.at[t])
                pair_copy(t).start()
                partial(2 * t + core, mine.at[t])

        i = tick - 1 - chip
        t = look_up(up, i)

        @pl.when((i >= 0) & (i < len(up)) & (look_up(owners, t) > chip))
        def _():
            fold_pair(t)

            @pl.when(chip > 0)
            def _():
                upward(t).wait_recv()
                mine[t] = mine[t] + from_low[t]

            upward(t).start()

        j = tick - 1 - (chips - 1 - chip)
        u = look_up(down, j)

        @pl.when((j >= 0) & (j < len(down)) & (look_up(owners, u) < chip))
        def _():
            fold_pair(u)

            @pl.when(chip < chips - 1)
            def _():
                downward(u).wait_recv()
                mine[u] = mine[u] + from_high[u]

            downward(u).start()

    place = look_up(places, chip)
    for slot in range(nown):
        t = slot * chips + place

        @pl.when(t < nhalf)
        def _():
            fold_pair(t)
            out[slot] = mine[t]

            @pl.when(chip > 0)
            def _():
                upward(t).wait_recv()
                out[slot] = out[slot] + from_low[t]

            @pl.when(chip < chips - 1)
            def _():
                downward(t).wait_recv()
                out[slot] = out[slot] + from_high[t]

        @pl.when(t >= nhalf)
        def _():
            rows, cols = square_iota()
            eye = jnp.where(rows == cols, 1.0, 0.0)
            pack_into(out.at[slot], eye, jnp.zeros((HALF, HALF), F32), eye)

    for t in range(nhalf):
        @pl.when(chip != owners[t])
        def _():
            upward(t).wait_send()


def dot3(a, b, contract):
    return jnp.stack([
        lax.dot_general(a[i], b[i], (contract, ((), ())), precision=HIGHEST, preferred_element_type=F32)
        for i in range(a.shape[0])
    ])


def sweep_inverse(a):
    count = a.shape[0]
    panel_shape = (count, 8, HALF)
    sub = lax.broadcasted_iota(jnp.int32, panel_shape, 1)
    lane = lax.broadcasted_iota(jnp.int32, panel_shape, 2)
    all_lanes = lax.broadcasted_iota(jnp.int32, (count, HALF, HALF), 2)

    def columns_of(top, first):
        return tuple(jnp.broadcast_to(top[:, :, k : k + 1], panel_shape) for k in range(first, first + 8))

    def panel(_, state):
        a, cols = state
        cols = list(cols)
        top = a[:, 0:8, :]
        for k in range(8):
            here = cols[k]
            inv = jnp.broadcast_to(1.0 / here[:, k : k + 1, :], panel_shape)
            row = jnp.broadcast_to(top[:, k : k + 1, :], panel_shape) * inv
            at_row = sub == k
            new = jnp.where(at_row, row, top - here * row)
            edge = jnp.where(at_row, inv, -here * inv)
            top = jnp.where(lane == k, edge, new)
            for j in range(k + 1, 8):
                across = jnp.broadcast_to(cols[j][:, k : k + 1, :], panel_shape) * inv
                cols[j] = jnp.where(at_row, across, cols[j] - here * across)
        top = jnp.where(lane < 8, -top, top)
        rest = a - jnp.stack([
            lax.dot_general(a[i, 0:8, :], top[i], (((0,), (0,)), ((), ())), precision=HIGHEST, preferred_element_type=F32)
            for i in range(count)
        ])
        ahead = columns_of(rest[:, 8:16, :], 8)
        tall = jnp.concatenate([top, jnp.zeros((count, HALF - 8, HALF), F32)], axis=1)
        turned = jnp.stack([tall[i].T for i in range(count)])
        rest = jnp.where(all_lanes < 8, turned, rest)
        a = jnp.concatenate([rest[:, 8:, :], top], axis=1)
        return pltpu.roll(a, HALF - 8, 2), ahead

    return -lax.fori_loop(0, HALF // 8, panel, (a, columns_of(a[:, 0:8, :], 0)), unroll=UNROLL)[0]


def invert_kernel(tokens, packed, out):
    count = packed.shape[0]
    rows, cols = square_iota()
    parts = [unpack(packed[i] / tokens) for i in range(count)]
    m11 = jnp.stack([p[0] for p in parts])
    m21 = jnp.stack([p[1] for p in parts])
    m22 = jnp.stack([p[2] for p in parts])
    eye = rows == cols
    trace = jnp.sum(jnp.where(eye, m11 + m22, 0.0), axis=(1, 2), keepdims=True)
    damping = jnp.where(eye, damping_ratio * trace / BLK, 0.0)
    x11 = sweep_inverse(m11 + damping)
    g = dot3(m21, x11, ((1,), (0,)))
    schur = m22 + damping - dot3(g, m21, ((1,), (1,)))
    y = sweep_inverse(schur)
    b21 = -dot3(y, g, ((1,), (0,)))
    b11 = x11 - dot3(g, b21, ((0,), (0,)))
    for i in range(count):
        pack_into(out.at[i], b11[i], b21[i], y[i])


def spread_kernel(n, sections, nhalf, nown, packed, full, rows_out, landed, low_s, high_s, near_r, pair_s, side_s, side_r):
    chips = n // 2
    share = BLK // n
    me = lax.axis_index("dp")
    section = lax.axis_index("pipe")
    core = lax.rem(me, 2)
    chip = me // 2
    pair = me + 1 - 2 * core
    low = (jnp.maximum(chip - 1, 0)) * 2 + core
    high = (jnp.minimum(chip + 1, chips - 1)) * 2 + core
    owners, places = owner_plan(chips, nhalf)

    greet(
        [(None, {"dp": pair}), (chip > 0, {"dp": low}), (chip < chips - 1, {"dp": high})]
        + [(None, {"pipe": lax.rem(section + step, sections)}) for step in range(1, sections)]
    )

    def send(source, t, half, target, sem):
        block = 2 * t + half
        return pltpu.make_async_remote_copy(
            src_ref=source, dst_ref=landed.at[block], send_sem=sem.at[t], recv_sem=near_r.at[block],
            device_id={"dp": target}, device_id_type=MESH,
        )

    def side(block, step):
        mine = full.at[block, pl.ds(pl.multiple_of(me * share, share), share), :]
        return pltpu.make_async_remote_copy(
            src_ref=mine, dst_ref=rows_out.at[section, block], send_sem=side_s.at[block, step - 1],
            recv_sem=side_r.at[section, block],
            device_id={"pipe": lax.rem(section + step, sections)}, device_id_type=MESH,
        )

    def open_block(value, block):
        m11, m21, m22 = unpack(value)
        full[block, 0:HALF, 0:HALF] = m11
        full[block, HALF:BLK, 0:HALF] = m21
        full[block, 0:HALF, HALF:BLK] = m21.T
        full[block, HALF:BLK, HALF:BLK] = m22
        for step in range(1, sections):
            side(block, step).start()
        rows_out[section, block] = full[block, pl.ds(pl.multiple_of(me * share, share), share), :]

    place = look_up(places, chip)
    for slot in range(nown):
        t = slot * chips + place

        @pl.when(t < nhalf)
        def _():
            @pl.when(chip > 0)
            def _():
                send(packed.at[slot], t, core, low, low_s).start()

            @pl.when(chip < chips - 1)
            def _():
                send(packed.at[slot], t, core, high, high_s).start()

            send(packed.at[slot], t, core, pair, pair_s).start()

    def arrived(t, half):
        send(landed.at[2 * t + half], t, half, pair, pair_s).wait_recv()

    def receive(t):
        arrived(t, core)
        source = landed.at[2 * t + core]

        @pl.when((look_up(owners, t) > chip) & (chip > 0))
        def _():
            send(source, t, core, low, low_s).start()

        @pl.when((look_up(owners, t) < chip) & (chip < chips - 1))
        def _():
            send(source, t, core, high, high_s).start()

        send(source, t, core, pair, pair_s).start()

    for slot in range(nown):
        t = slot * chips + place

        @pl.when(t < nhalf)
        def _():
            open_block(packed[slot], 2 * t + core)
            other = 2 * t + 1 - core
            arrived(t, 1 - core)
            open_block(landed[other], other)

    from_high = sorted(range(nhalf), key=lambda t: owners[t])
    from_low = sorted(range(nhalf), key=lambda t: -owners[t])
    below = sum((chip >= owner).astype(jnp.int32) for owner in owners)
    above = sum((chip <= owner).astype(jnp.int32) for owner in owners)

    @pl.loop(0, nhalf)
    def _(tick):
        i = tick + below
        t = look_up(from_high, i)
        j = tick + above
        u = look_up(from_low, j)

        @pl.when(i < nhalf)
        def _():
            receive(t)

        @pl.when(j < nhalf)
        def _():
            receive(u)

        for half in (core, 1 - core):
            for use, which in ((i < nhalf, t), (j < nhalf, u)):
                @pl.when(use)
                def _():
                    block = 2 * which + half
                    if half is not core:
                        arrived(which, half)
                    open_block(landed[block], block)

    for t in range(nhalf):
        owner = owners[t]
        source = landed.at[2 * t + core]

        @pl.when((chip > 0) & (chip <= owner))
        def _():
            send(source, t, core, low, low_s).wait_send()

        @pl.when((chip < chips - 1) & (chip >= owner))
        def _():
            send(source, t, core, high, high_s).wait_send()

        send(source, t, core, pair, pair_s).wait_send()

    @pl.loop(0, 2 * nhalf)
    def _(block):
        for step in range(1, sections):
            side(block, step).wait_send()
            source = lax.rem(section + step, sections)
            pltpu.make_async_remote_copy(
                src_ref=rows_out.at[source, block], dst_ref=rows_out.at[source, block],
                send_sem=side_s.at[block, step - 1], recv_sem=side_r.at[source, block],
                device_id={"pipe": source}, device_id_type=MESH,
            ).wait_recv()


def apply_kernel(per_step, owners, inverse, grad, rows, precond, held, slots):
    step = pl.program_id(0)
    section = lax.axis_index("pipe")
    sections, nblocks = owners.shape
    total = sections * nblocks

    @pl.when(step == 0)
    def _():
        for j in range(HOST):
            slots[j] = -1

        def place(k, used):
            hit = owners[k // nblocks, lax.rem(k, nblocks)] == section

            @pl.when(hit)
            def _():
                slots[used] = k

            return used + hit.astype(jnp.int32)

        lax.fori_loop(0, total, place, jnp.int32(0))

    for j in range(per_step):
        k = slots[step * per_step + j]
        at = jnp.maximum(k, 0)
        value = rows[at // nblocks, lax.rem(at, nblocks)]
        held[j] = jnp.where(k >= 0, value, 0.0)

    for i in range(inverse.shape[0]):
        span = slice(i * BLK, (i + 1) * BLK)
        a = inverse[i]
        b = grad[span, :]
        a_high = a.astype(BF16)
        a_low = (a - a_high.astype(F32)).astype(BF16)
        b_high = b.astype(BF16)
        b_low = (b - b_high.astype(F32)).astype(BF16)
        left = jnp.concatenate([a_high, a_low, a_high], axis=1)
        right = jnp.concatenate([b_low, b_high, b_high], axis=0)
        precond[span, :] = jnp.dot(left, right, preferred_element_type=F32)


def shards(acts, grad, owner_of):
    tokens, feature_count = acts.shape[1:]
    columns = grad.shape[1]
    nblocks = feature_count // BLK
    n = lax.axis_size("dp")
    sections = lax.axis_size("pipe")
    chips = n // 2
    nhalf = nblocks // 2
    nown = -(-nhalf // chips)
    share = BLK // n
    vmem = pl.BlockSpec(memory_space=pltpu.VMEM)
    dma = pltpu.SemaphoreType.DMA

    summed = pl.pallas_call(
        functools.partial(reduce_kernel, n, nhalf, nown),
        out_shape=jax.ShapeDtypeStruct((nown, PACK, BLK), F32),
        in_specs=[vmem],
        out_specs=vmem,
        scratch_shapes=[
            pltpu.VMEM((nhalf, PACK, BLK), F32),
            pltpu.VMEM((nhalf, PACK, BLK), F32),
            pltpu.VMEM((nhalf, PACK, BLK), F32),
            pltpu.VMEM((nhalf, PACK, BLK), F32),
            pltpu.VMEM((nhalf, PACK, BLK), F32),
            dma((nhalf,)), dma((nhalf,)), dma((nhalf,)), dma((nhalf,)), dma((nhalf,)),
        ],
        compiler_params=pltpu.CompilerParams(collective_id=0, has_side_effects=True),
        name="reduce_factors",
    )(acts[0])

    packed = pl.pallas_call(
        functools.partial(invert_kernel, float(tokens * n)),
        out_shape=jax.ShapeDtypeStruct((nown, PACK, BLK), F32),
        in_specs=[vmem],
        out_specs=vmem,
        name="invert_blocks",
    )(summed)

    inverse, rows = pl.pallas_call(
        functools.partial(spread_kernel, n, sections, nhalf, nown),
        out_shape=(
            jax.ShapeDtypeStruct((nblocks, BLK, BLK), F32),
            jax.ShapeDtypeStruct((sections, nblocks, share, BLK), F32),
        ),
        in_specs=[vmem],
        out_specs=(vmem, vmem),
        scratch_shapes=[
            pltpu.VMEM((nblocks, PACK, BLK), F32),
            dma((nhalf,)), dma((nhalf,)), dma((nblocks,)), dma((nhalf,)),
            dma((nblocks, sections - 1)), dma((sections, nblocks)),
        ],
        compiler_params=pltpu.CompilerParams(collective_id=1, has_side_effects=True),
        name="spread_inverses",
    )(packed)

    group = 2 if nblocks % 2 == 0 else 1
    per_step = HOST // (nblocks // group)
    precond, held = pl.pallas_call(
        functools.partial(apply_kernel, per_step),
        grid_spec=pltpu.PrefetchScalarGridSpec(
            num_scalar_prefetch=1,
            grid=(nblocks // group,),
            in_specs=[
                pl.BlockSpec((group, BLK, BLK), lambda i, o: (i, 0, 0)),
                pl.BlockSpec((group * BLK, columns), lambda i, o: (i, 0)),
                pl.BlockSpec((sections, nblocks, share, BLK), lambda i, o: (0, 0, 0, 0), pipeline_mode=pl.Buffered(1)),
            ],
            out_specs=[
                pl.BlockSpec((group * BLK, columns), lambda i, o: (i, 0)),
                pl.BlockSpec((per_step, share, BLK), lambda i, o: (i, 0, 0)),
            ],
            scratch_shapes=[pltpu.SMEM((HOST,), jnp.int32)],
        ),
        out_shape=(
            jax.ShapeDtypeStruct((feature_count, columns), F32),
            jax.ShapeDtypeStruct((HOST, share, BLK), F32),
        ),
        compiler_params=pltpu.CompilerParams(dimension_semantics=("arbitrary",)),
        name="apply_inverses",
    )(owner_of, inverse, grad, rows)
    return precond, held[None]


def solution(mesh):
    placed = (P("pipe", "dp", None), P("pipe", "dp"), P())
    return jax.shard_map(
        shards,
        mesh=mesh,
        in_specs=placed,
        out_specs=(P("pipe", "dp"), P("pipe", None, "dp", None)),
        check_vma=False,
    )
```
